32 devices in a mesh: ctx: 2 (over y), tp: 2 (over core), dec: 8 (over z, x).
Axes of the slice: x: 2, y: 2, z: 4, core: 2. Of those that a mesh axis runs over, the one named last changes fastest.
Arguments:
- cache: bfloat16 [8, 512, 576], P('dec', 'ctx'), may hold values from -6 to 6
- lengths: int32 [8], P('dec'), may hold values from 1 to 512
- slot_sequence: int32 [8], replicated, may hold values from 0 to 7, each once
- parents: int32 [8, 64], P('dec'), may hold values from 0 to 62, as said below
- query_nope: bfloat16 [8, 64, 128, 128], P('dec', None, 'tp'), may hold values from -6 to 6
- query_rope: bfloat16 [8, 64, 128, 64], P('dec', None, 'tp'), may hold values from -90 to 90
- new_latent: bfloat16 [8, 64, 576], P('dec'), may hold values from -6 to 6
- key_up: bfloat16 [128, 128, 512], P('tp'), may hold values from -0.5 to 0.5
- value_up: bfloat16 [128, 512, 128], P('tp'), may hold values from -0.25 to 0.25
- out_proj: bfloat16 [16384, 7168], P('tp', ('ctx', 'dec')), may hold values from -0.046875 to 0.046875
Outputs:
- attended: bfloat16 [8, 64, 7168], P(None, 'tp', ('ctx', 'dec'))
The draws below stay inside these ranges and needn't reach their ends.
Inputs may be any that keep to these rules, and one draw needn't show every extreme that they name: `slot_sequence`: every sequence is held by exactly one slot. parents[s, 0] = 0 and parents[s, i] < i for every i >= 1.
All inputs are finite; a program needn't handle non-finite values.
Results may differ from the reference program's by a relative error of at most 0.024.
Values may be sent and summed in bfloat16 or wider, within the bound.
No kernel may reach another device: no remote copies, remote signals or barrier semaphores. Data moves between devices by JAX's collectives and lax.ppermute only.
A program may use at most 128 MiB of HBM per device.

```python
import math
import jax
import jax.numpy as jnp
from jax import lax

D = 7168
H = 128
HD = 128
RD = 64
LAT = 512
VD = 128
NODES = 64
SEQS = 8
CACHE = 512


def shared_tree(key):
    latent_key, rope_key = jax.random.split(key, 2)
    latent_rows = jnp.clip(jax.random.normal(latent_key, (SEQS, NODES, LAT + RD), jnp.float32), -6.0, 6.0)
    rope_rows = jnp.clip(jax.random.normal(rope_key, (SEQS, NODES, H, RD), jnp.float32), -6.0, 6.0)
    return (latent_rows, rope_rows)


def draw_new_latent(key, part):
    return shared_tree(jax.random.fold_in(key, 7))[0].astype(jnp.bfloat16)


def draw_query_rope(key, part):
    return shared_tree(jax.random.fold_in(key, 7))[1].astype(jnp.bfloat16)


def draw_parents(key, part):
    node_ids = jnp.arange(NODES, dtype=jnp.int32)
    upper = jnp.broadcast_to(jnp.maximum(node_ids, 1)[None, :], (SEQS, NODES))
    return jax.random.randint(key, (SEQS, NODES), 0, upper).astype(jnp.int32)


def set_ends(array, own_key, low, largest):
    spot = [jax.random.randint(jax.random.fold_in(own_key, axis), (), 0, length) for axis, length in enumerate(array.shape)]
    widest = array.shape.index(max(array.shape))
    beside = spot[:widest] + [(spot[widest] + 1) % array.shape[widest]] + spot[widest + 1:]
    return array.at[tuple(spot)].set(low).at[tuple(beside)].set(largest)


def block_levels(rng, dims, pieces, smallest, high):
    level = 1.0
    for position, parts in pieces:
        steps = jax.random.uniform(jax.random.fold_in(jax.random.fold_in(rng, 6), position), (parts,), jnp.float32, smallest / len(pieces), high / len(pieces))
        level = level * jnp.repeat(jnp.exp(steps), dims[position] // parts).reshape((-1,) + (1,) * (len(dims) - 1 - position))
    return level


def gaussian(key, shape, deviation, bound, cuts=(), held_as=jnp.bfloat16):
    values = jax.random.normal(key, shape, jnp.float32) * deviation
    if len(cuts) > 0:
        values = block_levels(key, shape, cuts, -0.22, 0.18) * values
    return jnp.clip(values, min=-bound, max=bound).astype(held_as)


def setup_inputs(seed: int = 0) -> dict:
    key_of = jax.random.split(jax.random.key(seed), 11)
    cache = gaussian(key_of[0], (SEQS, CACHE, LAT + RD), 1.0, 6.0, ((0, 8), (1, 2)))
    lengths = set_ends(jax.random.randint(key_of[1], (SEQS,), 1, CACHE + 1), jax.random.fold_in(key_of[1], 1), 1, CACHE).astype(jnp.int32)
    slot_sequence = jax.random.permutation(key_of[2], SEQS).astype(jnp.int32)
    parents = draw_parents(jax.random.fold_in(key_of[10], 71), 0)
    query_nope = gaussian(key_of[4], (SEQS, NODES, H, HD), 1.0, 6.0, ((0, 8), (2, 2)))
    query_rope = draw_query_rope(jax.random.fold_in(key_of[10], 71), 0)
    new_latent = draw_new_latent(jax.random.fold_in(key_of[10], 71), 0)
    key_up = gaussian(key_of[7], (H, HD, LAT), HD ** -0.5, 0.5, ((0, 2),))
    value_up = gaussian(key_of[8], (H, LAT, VD), LAT ** -0.5, 0.25, ((0, 2),))
    out_proj = gaussian(key_of[9], (H * VD, D), (H * VD) ** -0.5, 0.046875, ((0, 2), (1, 16)))
    return {"cache": cache, "lengths": lengths, "slot_sequence": slot_sequence, "parents": parents, "query_nope": query_nope, "query_rope": query_rope, "new_latent": new_latent, "key_up": key_up, "value_up": value_up, "out_proj": out_proj}


def ancestors(parents):
    node_count = parents.shape[-1]
    node_ids = jnp.arange(node_count, dtype=jnp.int32)
    parent_link = (parents[..., :, None] == node_ids).astype(jnp.float32)
    closure = jnp.maximum(parent_link, jnp.eye(node_count, dtype=jnp.float32))
    for _ in range(node_count.bit_length()):
        closure = jnp.minimum(jnp.einsum('sij,sjk->sik', closure, closure, precision=lax.Precision.HIGHEST), 1.0)
    return closure

def reference(cache, lengths, slot_sequence, parents, query_nope, query_rope, new_latent, key_up, value_up, out_proj):
    score_scale = 1.0 / math.sqrt(HD + RD)
    tree_mask = ancestors(parents)
    positions = jnp.arange(CACHE, dtype=jnp.int32)
    key_weight = key_up.astype(jnp.float32)
    value_weight = value_up.astype(jnp.float32)

    def per_slot(slot_index):
        sequence = slot_sequence[slot_index]
        cache_rows = lax.dynamic_index_in_dim(cache, sequence, 0, keepdims=False).astype(jnp.float32)
        length = lax.dynamic_index_in_dim(lengths, sequence, 0, keepdims=False)
        absorbed = jnp.einsum('nhd,hdc->nhc', query_nope[slot_index].astype(jnp.float32), key_weight).astype(jnp.bfloat16)
        queries = lax.optimization_barrier(jnp.concatenate([absorbed, query_rope[slot_index]], axis=-1)).astype(jnp.float32)
        tree_rows = new_latent[slot_index].astype(jnp.float32)
        cache_scores = jnp.einsum('nhc,pc->nhp', queries, cache_rows) * score_scale
        tree_scores = jnp.einsum('nhc,pc->nhp', queries, tree_rows) * score_scale
        cache_live = (positions < length)[None, None, :]
        tree_live = (tree_mask[slot_index] > 0)[:, None, :]
        cache_scores = jnp.where(cache_live, cache_scores, -1e+30)
        tree_scores = jnp.where(tree_live, tree_scores, -1e+30)
        row_peak = jnp.maximum(lax.optimization_barrier(jnp.max(cache_scores, axis=-1)), lax.optimization_barrier(jnp.max(tree_scores, axis=-1)))
        cache_expo = jnp.where(cache_live, jnp.exp(cache_scores - row_peak[..., None]), 0.0)
        tree_expo = jnp.where(tree_live, jnp.exp(tree_scores - row_peak[..., None]), 0.0)
        row_total = lax.optimization_barrier(jnp.sum(cache_expo, axis=-1)) + lax.optimization_barrier(jnp.sum(tree_expo, axis=-1))
        cache_weights = lax.optimization_barrier(cache_expo.astype(jnp.bfloat16)).astype(jnp.float32)
        tree_weights = lax.optimization_barrier(tree_expo.astype(jnp.bfloat16)).astype(jnp.float32)
        weighted = jnp.einsum('nhp,pc->nhc', cache_weights, cache_rows[:, :LAT])
        weighted = weighted + jnp.einsum('nhp,pc->nhc', tree_weights, tree_rows[:, :LAT])
        latent_out = weighted / row_total[..., None]
        return jnp.einsum('nhc,hcv->nhv', latent_out, value_weight, precision=lax.Precision.HIGHEST).astype(jnp.bfloat16)
    head_out = lax.map(per_slot, jnp.arange(SEQS, dtype=jnp.int32))
    flat_rows = head_out.reshape(SEQS * NODES, H * VD)
    attended = jnp.dot(flat_rows, out_proj, preferred_element_type=jnp.float32).astype(jnp.bfloat16)
    return attended.reshape(SEQS, NODES, D)
```

```python
import math

import jax
import jax.numpy as jnp
from jax import lax
from jax.experimental import pallas as pl
from jax.experimental.pallas import tpu as pltpu
from jax.sharding import PartitionSpec as P

NEG = -1e30
F32 = jnp.float32
BF16 = jnp.bfloat16
NT = (((1,), (1,)), ((), ()))


def bit_list(count):
    return [1 << k for k in range(count.bit_length() - 1)]


def swap(value, axis, mask):
    count = lax.axis_size(axis)
    return lax.ppermute(value, axis, [(i, i ^ mask) for i in range(count)])


def round_up(value, unit):
    return -(-value // unit) * unit


def tree_kernel(spots_ref, parents_ref, latent_ref, out_ref):
    nodes, feat = latent_ref.shape
    extra = out_ref.shape[1] - feat
    first = spots_ref[0]
    block = spots_ref[1]
    row = lax.broadcasted_iota(jnp.int32, (nodes, nodes), 0)
    col = lax.broadcasted_iota(jnp.int32, (nodes, nodes), 1)
    linked = (parents_ref[...] == row) | (row == col)
    closure = jnp.where(linked, 1.0, 0.0)
    for _ in range((nodes - 1).bit_length()):
        packed = closure.astype(BF16)
        closure = jnp.minimum(jnp.dot(packed, packed, preferred_element_type=F32), 1.0)
    row = lax.broadcasted_iota(jnp.int32, (nodes, extra), 0)
    col = lax.broadcasted_iota(jnp.int32, (nodes, extra), 1)
    pick = jnp.where(row == first + col - 1, 1.0, 0.0).astype(BF16)
    seen = jnp.dot(closure.astype(BF16), pick, preferred_element_type=F32)
    barred = (col >= 1) & (col <= block) & (seen < 0.5)
    out_ref[:, :feat] = latent_ref[...]
    out_ref[:, feat:] = jnp.where(barred, NEG, 0.0).astype(BF16)


def absorb_kernel(nope_ref, rope_ref, key_up_ref, out_ref):
    heads, nodes, _ = nope_ref.shape
    latent = key_up_ref.shape[2]
    feat = latent + rope_ref.shape[2]
    extra = out_ref.shape[2] - feat
    row = lax.broadcasted_iota(jnp.int32, (nodes, extra), 0)
    col = lax.broadcasted_iota(jnp.int32, (nodes, extra), 1)
    marks = jnp.where((col == 0) | (col == row + 1), 1.0, 0.0).astype(BF16)
    for h in range(heads):
        absorbed = jnp.dot(nope_ref[h], key_up_ref[h], preferred_element_type=F32)
        out_ref[h, :, :latent] = absorbed.astype(BF16)
        out_ref[h, :, latent:feat] = rope_ref[h]
        out_ref[h, :, feat:] = marks


def attend_kernel(score_scale, *refs):
    query_ref, tree_ref, value_ref = refs[:3]
    key_refs = refs[3:-1]
    out_ref = refs[-1]
    heads, nodes, width = query_ref.shape
    latent = value_ref.shape[1]
    depth = value_ref.shape[2]
    queries = query_ref[...].reshape(heads * nodes, width)
    scores = [jnp.dot(queries, key_ref[...], preferred_element_type=F32) for key_ref in key_refs]
    scores.append(lax.dot_general(queries, tree_ref[...], NT, preferred_element_type=F32))
    peak = scores[0].max(axis=-1, keepdims=True)
    for part in scores[1:]:
        peak = jnp.maximum(peak, part.max(axis=-1, keepdims=True))
    factor = score_scale * math.log2(math.e)
    expos = [jnp.exp2((part - peak) * factor) for part in scores]
    total = expos[0].sum(axis=-1, keepdims=True)
    for part in expos[1:]:
        total = total + part.sum(axis=-1, keepdims=True)
    weighted = jnp.dot(expos[-1].astype(BF16), tree_ref[:, :latent], preferred_element_type=F32)
    for part, key_ref in zip(expos, key_refs):
        weighted = weighted + lax.dot_general(
            part.astype(BF16), key_ref[:latent, :], NT, preferred_element_type=F32
        )
    weighted = weighted.astype(BF16)
    share = 1.0 / total
    for h in range(heads):
        rows = slice(h * nodes, (h + 1) * nodes)
        projected = jnp.dot(weighted[rows], value_ref[h], preferred_element_type=F32)
        out_ref[:, h * depth : (h + 1) * depth] = (projected * share[rows]).astype(BF16)


def project_kernel(*refs):
    part_refs, weight_ref, out_ref = refs[:-2], refs[-2], refs[-1]
    rows = jnp.concatenate([ref[...] for ref in part_refs], axis=0)
    product = lax.dot_general(rows, weight_ref[...], NT, preferred_element_type=F32)

    @pl.when(pl.program_id(0) == 0)
    def _():
        out_ref[...] = product

    @pl.when(pl.program_id(0) > 0)
    def _():
        out_ref[...] += product


def collect_kernel(places, block, spots_ref, *refs):
    out_ref = refs[-1]
    for (dec_mask, ctx_mask), entries in places.items():
        total = None
        for index, offset in entries:
            part = refs[index][offset : offset + block, :]
            total = part if total is None else total + part
        slot = spots_ref[0] ^ dec_mask
        first = pl.multiple_of((spots_ref[1] ^ ctx_mask) * block, block)
        out_ref[slot, pl.ds(first, block), :] = total


def whole_spec(shape):
    return pl.BlockSpec(shape, lambda *_: (0,) * len(shape))


SMEM_SPEC = pl.BlockSpec(memory_space=pltpu.SMEM)


def on_device(
    cache,
    lengths,
    slot_sequence,
    parents,
    query_nope,
    query_rope,
    new_latent,
    key_up,
    value_up,
    out_proj,
):
    ctx_count = lax.axis_size("ctx")
    dec_count = lax.axis_size("dec")
    tp_count = lax.axis_size("tp")
    ctx_at = lax.axis_index("ctx")
    dec_at = lax.axis_index("dec")
    tp_at = lax.axis_index("tp")
    rows = cache.shape[1]
    feat = cache.shape[2]
    heads, head_size, latent = key_up.shape
    depth = value_up.shape[2]
    nodes = parents.shape[1]
    node_block = nodes // ctx_count
    first_node = ctx_at * node_block
    columns = out_proj.shape[1]
    width = round_up(feat + 1 + node_block, 128)
    score_scale = 1.0 / math.sqrt(head_size + feat - latent)
    row_block = rows // tp_count

    positions = ctx_at * rows + jnp.arange(rows, dtype=jnp.int32)
    bias = jnp.where(positions < lengths[0], 0.0, NEG).astype(BF16)[None, :]
    keys = jnp.concatenate([cache[0].T, bias, jnp.zeros((width - feat - 1, rows), BF16)], axis=0)
    keys = lax.dynamic_slice_in_dim(keys, tp_at * row_block, row_block, 1)
    pieces = keys.reshape(dec_count, width // dec_count, row_block)
    pieces = lax.all_to_all(pieces, "dec", 0, 0, tiled=True)
    pieces = jnp.stack(
        [lax.dynamic_index_in_dim(pieces, slot_sequence[k], 0, False) for k in range(dec_count)]
    )
    pieces = lax.all_to_all(pieces, "dec", 0, 0, tiled=True)
    keys = pieces.reshape(width, row_block)
    for mask in bit_list(ctx_count):
        keys = jnp.concatenate([keys, swap(keys, "ctx", mask)], axis=1)
    key_parts = [keys]
    for mask in bit_list(tp_count):
        sent = keys if len(key_parts) == 1 else jnp.concatenate(key_parts, axis=1)
        key_parts = [sent, swap(sent, "tp", mask)]

    spots = jnp.stack([first_node, jnp.int32(node_block)])
    tree = pl.pallas_call(
        tree_kernel,
        in_specs=[SMEM_SPEC, whole_spec((1, nodes)), whole_spec((nodes, feat))],
        out_specs=whole_spec((nodes, width)),
        out_shape=jax.ShapeDtypeStruct((nodes, width), BF16),
        grid=(1,),
        name="tree_keys",
    )(spots, parents, new_latent[0])

    head_step = min(8, heads)
    nope = lax.dynamic_slice_in_dim(query_nope[0], first_node, node_block, 0).transpose(1, 0, 2)
    rope = lax.dynamic_slice_in_dim(query_rope[0], first_node, node_block, 0).transpose(1, 0, 2)
    queries = pl.pallas_call(
        absorb_kernel,
        grid=(heads // head_step,),
        in_specs=[
            pl.BlockSpec((head_step, node_block, head_size), lambda i: (i, 0, 0)),
            pl.BlockSpec((head_step, node_block, feat - latent), lambda i: (i, 0, 0)),
            pl.BlockSpec((head_step, head_size, latent), lambda i: (i, 0, 0)),
        ],
        out_specs=pl.BlockSpec((head_step, node_block, width), lambda i: (i, 0, 0)),
        out_shape=jax.ShapeDtypeStruct((heads, node_block, width), BF16),
        cost_estimate=pl.CostEstimate(
            flops=4 * heads * node_block * head_size * latent,
            bytes_accessed=2 * heads * head_size * latent,
            transcendentals=0,
        ),
        name="absorb",
    )(nope, rope, key_up)

    class_heads = heads // 2
    step = min(head_step, class_heads)
    key_rows = sum(part.shape[1] for part in key_parts)

    def attend(which):
        base = which * (class_heads // step)
        return pl.pallas_call(
            lambda *refs: attend_kernel(score_scale, *refs),
            grid=(class_heads // step,),
            in_specs=[
                pl.BlockSpec((step, node_block, width), lambda i: (base + i, 0, 0)),
                whole_spec((nodes, width)),
                pl.BlockSpec((step, latent, depth), lambda i: (base + i, 0, 0)),
            ]
            + [whole_spec(part.shape) for part in key_parts],
            out_specs=pl.BlockSpec((node_block, step * depth), lambda i: (0, i)),
            out_shape=jax.ShapeDtypeStruct((node_block, class_heads * depth), BF16),
            cost_estimate=pl.CostEstimate(
                flops=2 * class_heads * node_block * (key_rows + nodes) * (width + latent),
                bytes_accessed=2 * class_heads * latent * depth,
                transcendentals=class_heads * node_block * key_rows,
            ),
            name="attend_%d" % which,
        )(queries, tree, value_up, *key_parts)

    dec_bits = [("dec", bit) for bit in bit_list(dec_count)]
    ctx_bits = [("ctx", bit) for bit in bit_list(ctx_count)]
    orders = (
        dec_bits[2:] + dec_bits[:1] + dec_bits[1:2] + ctx_bits,
        dec_bits[2:] + ctx_bits + dec_bits[1:2] + dec_bits[:1],
    )

    weight = out_proj.T
    class_depth = class_heads * depth
    depth_step = min(1024, class_depth)
    depth_steps = class_depth // depth_step

    def project(parts, which):
        count = len(parts)
        return pl.pallas_call(
            project_kernel,
            grid=(depth_steps,),
            in_specs=[pl.BlockSpec((node_block, depth_step), lambda i: (0, i))] * count
            + [pl.BlockSpec((columns, depth_step), lambda i: (0, which * depth_steps + i))],
            out_specs=whole_spec((count * node_block, columns)),
            out_shape=jax.ShapeDtypeStruct((count * node_block, columns), F32),
            cost_estimate=pl.CostEstimate(
                flops=2 * count * node_block * class_depth * columns,
                bytes_accessed=2 * class_depth * columns,
                transcendentals=0,
            ),
            name="project_%d" % which,
        )(*parts, weight)

    places = {}
    results = []
    waves = []
    held = [{(0, 0): attend(which)} for which in range(2)]
    for level in range(len(orders[0])):
        for which in range(2):
            axis, mask = orders[which][level]
            fresh = {}
            for (dec_mask, ctx_mask), part in held[which].items():
                spot = (dec_mask ^ mask, ctx_mask) if axis == "dec" else (dec_mask, ctx_mask ^ mask)
                fresh[spot] = swap(part, axis, mask)
            if level == len(orders[0]) - 1:
                waves.append((which, held[which]))
                waves.append((which, fresh))
            held[which] = {**held[which], **fresh}
    for which, parts in waves:
        index = len(results)
        results.append(project(list(parts.values()), which))
        for k, spot in enumerate(parts):
            places.setdefault(spot, []).append((index, k * node_block))

    here = jnp.stack([dec_at, ctx_at])
    partial = pl.pallas_call(
        lambda *refs: collect_kernel(places, node_block, *refs),
        in_specs=[SMEM_SPEC] + [whole_spec(part.shape) for part in results],
        out_specs=whole_spec((dec_count, nodes, columns)),
        out_shape=jax.ShapeDtypeStruct((dec_count, nodes, columns), F32),
        grid=(1,),
        name="collect",
    )(here, *results)
    if tp_count != 2:
        return lax.psum_scatter(partial.astype(BF16), "tp", scatter_dimension=1, tiled=True)
    half = nodes // 2
    away = lax.dynamic_slice_in_dim(partial, (1 - tp_at) * half, half, 1).astype(BF16)
    kept = lax.dynamic_slice_in_dim(partial, tp_at * half, half, 1)
    return (kept + swap(away, "tp", 1).astype(F32)).astype(BF16)


def solution(mesh):
    return jax.shard_map(
        on_device,
        mesh=mesh,
        in_specs=(
            P("dec", "ctx", None),
            P("dec"),
            P(),
            P("dec", None),
            P("dec", None, "tp", None),
            P("dec", None, "tp", None),
            P("dec", None, None),
            P("tp", None, None),
            P("tp", None, None),
            P("tp", ("ctx", "dec")),
        ),
        out_specs=P(None, "tp", ("ctx", "dec")),
        check_vma=False,
    )
```
